32 devices in a mesh: morton: 8 (over y, x, core), group: 4 (over z).
Axes of the slice: x: 2, y: 2, z: 4, core: 2. Of those that a mesh axis runs over, the one named last changes fastest.
Arguments:
- state: float32 [4, 64, 5, 512], P('group', 'morton'), may hold values from -12 to 110, as said below
- patch_count: int32 [8], P('morton'), may hold values from 1 to 8, as said below
- neighbour_table: int32 [8, 8, 4], P('morton'), may hold values from -1 to 63, as said below
- send_table: int32 [8, 8, 5], P('morton'), may hold values from -1 to 31, as said below
- ghost_table: int32 [8, 8, 4], P('morton'), may hold values from -1 to 39, as said below
Outputs:
- updated: float32 [4, 64, 5, 512], P('group', 'morton')
The draws below stay inside these ranges and needn't reach their ends.
Inputs may be any that keep to these rules, and one draw needn't show every extreme that they name: `state`: density lies in [0.5, 2] and the pressure implied by the five variables in [0.1, 0.4] in every live cell. `patch_count`: range i holds slab-order positions starting[i] to starting[i+1] - 1, where starting[i] = i * 4 + j[i] with |j[i]| <= 2 and j[0] = j[8] = 0; some range holds 8. `neighbour_table`: global slot = range * 8 + local slot; slab positions form rows of 4; faces 0 and 1 meet positions -4 and +4, faces 2 and 3 the neighbours in the row; empty slots and domain walls give -1. `send_table`: entry [i, j, t] is -1 or local slot * 4 + face of a patch of range i whose face goes to slot t of the message from i to j; messages of some pair use all 5 slots. `ghost_table`: -1 for faces whose neighbour is held by the same range or absent; else i * 5 + t for the face sent by range i in slot t, and i lies within 2 of the receiving range.
All inputs are finite; a program needn't handle non-finite values.
Results may differ from the reference program's by a relative error of at most 0.00002.
Values sent between devices are 32-bit elements; how exact they have to be, the bound alone decides.
A program may use at most 64 MiB of HBM per device.

```python
import jax
import jax.numpy as jnp
from jax import lax

EDGE = 8
VARS = 5
PATCH_DEV = 4
RANGES = 8
SLABS = 4
SLOTS = 8
MSG_SLOTS = 5
CELLS = 512


def layout(key):
    half = PATCH_DEV // 2
    jitter = jax.random.randint(jax.random.fold_in(key, 11), (RANGES + 1,), -half + 1, half)
    chosen = jax.random.randint(jax.random.fold_in(key, 12), (), 1, RANGES - 2)
    marks = jnp.arange(RANGES + 1, dtype=jnp.int32)
    jitter = jnp.where(marks == chosen, -half, jitter)
    jitter = jnp.where((marks == chosen + 1) | (marks == chosen + 2), half, jitter)
    jitter = jnp.where((marks == 0) | (marks == RANGES), 0, jitter)
    starts = (marks * PATCH_DEV + jitter).astype(jnp.int32)
    counts = (starts[1:] - starts[:-1]).astype(jnp.int32)
    total = RANGES * PATCH_DEV
    slot_ids = jnp.arange(SLOTS, dtype=jnp.int32)
    places = starts[:-1, None] + slot_ids[None, :]
    filled = slot_ids[None, :] < counts[:, None]
    offsets = jnp.array([-PATCH_DEV, PATCH_DEV, -1, 1], dtype=jnp.int32)
    target = places[:, :, None] + offsets
    column = places % PATCH_DEV
    always = jnp.ones_like(filled)
    inside = (target >= 0) & (target < total)
    inside = inside & jnp.stack([always, always, column > 0, column < PATCH_DEV - 1], axis=-1)
    inside = inside & filled[:, :, None]
    clipped = jnp.clip(target, 0, total - 1)
    owners = jnp.sum((clipped[..., None] >= starts[1:RANGES]).astype(jnp.int32), axis=-1).astype(jnp.int32)
    local = (clipped - starts[owners]).astype(jnp.int32)
    neighbour = jnp.where(inside, owners * SLOTS + local, -1).astype(jnp.int32)
    home = jnp.arange(RANGES, dtype=jnp.int32)[:, None, None]
    remote = inside & (owners != home)
    flat_remote = remote.reshape(RANGES, SLOTS * 4)
    flat_owner = owners.reshape(RANGES, SLOTS * 4)
    onehot = (flat_remote[:, :, None] & (flat_owner[:, :, None] == jnp.arange(RANGES, dtype=jnp.int32))).astype(jnp.int32)
    running = jnp.cumsum(onehot, axis=1) - 1
    message_slot = jnp.sum(onehot * running, axis=-1).reshape(RANGES, SLOTS, 4).astype(jnp.int32)
    ghost = jnp.where(remote, owners * MSG_SLOTS + message_slot, -1).astype(jnp.int32)
    directions = jnp.arange(4, dtype=jnp.int32)
    opposite = directions + 1 - 2 * (directions % 2)
    face_id = (local * 4 + opposite).astype(jnp.int32)
    sender = jnp.where(remote, owners, RANGES)
    receiver = jnp.broadcast_to(home, sender.shape)
    table = jnp.full((RANGES, RANGES, MSG_SLOTS), -1, dtype=jnp.int32)
    table = table.at[sender, receiver, message_slot].set(face_id, mode='drop')
    return (counts, neighbour, table, ghost)


def draw_patch_count(key, part):
    return layout(key)[0]


def draw_neighbour_table(key, part):
    return layout(key)[1]


def draw_send_table(key, part):
    return layout(key)[2]


def draw_ghost_table(key, part):
    return layout(key)[3]


def draw_state(key, part):
    count_all = RANGES * SLOTS
    shape = (SLABS, count_all, 1, CELLS)
    slab = jnp.arange(SLABS, dtype=jnp.int32)[:, None, None, None]
    slot = jnp.arange(count_all, dtype=jnp.int32)[None, :, None, None]
    rise = (slot // SLOTS * SLABS + slab).astype(jnp.float32) / (RANGES * SLABS - 1)
    density = jnp.exp(jax.random.uniform(jax.random.fold_in(key, 1), shape, jnp.float32, jnp.log(0.5), jnp.log(2.0)))
    pressure = jnp.exp(jax.random.uniform(jax.random.fold_in(key, 2), shape, jnp.float32, jnp.log(0.1), jnp.log(0.4)))
    vshape = (SLABS, count_all, 3, CELLS)
    velocity = 0.5 * (1.0 + 3.0 * rise) * jnp.clip(jax.random.normal(jax.random.fold_in(key, 3), vshape, jnp.float32), -3.0, 3.0)
    momenta = density * velocity
    energy = pressure / 0.4 + 0.5 * density * jnp.sum(velocity * velocity, axis=2, keepdims=True)
    return jnp.concatenate([density, momenta, energy], axis=2).astype(jnp.float32)


def setup_inputs(seed: int = 0) -> dict:
    seeds = jax.random.split(jax.random.key(seed), 6)
    return {
        "state": draw_state(jax.random.fold_in(seeds[5], 71), 0),
        "patch_count": draw_patch_count(jax.random.fold_in(seeds[5], 71), 0),
        "neighbour_table": draw_neighbour_table(jax.random.fold_in(seeds[5], 71), 0),
        "send_table": draw_send_table(jax.random.fold_in(seeds[5], 71), 0),
        "ghost_table": draw_ghost_table(jax.random.fold_in(seeds[5], 71), 0),
    }


GAMMA = 1.4
COURANT = 0.8

def face_layer(blocks, direction):
    if direction == 0:
        return blocks[..., 0, :, :]
    if direction == 1:
        return blocks[..., -1, :, :]
    if direction == 2:
        return blocks[..., :, 0, :]
    if direction == 3:
        return blocks[..., :, -1, :]
    if direction == 4:
        return blocks[..., :, :, 0]
    return blocks[..., :, :, -1]

def primitives(blocks):
    density = blocks[..., 0, :, :, :]
    momenta = blocks[..., 1:4, :, :, :]
    energy = blocks[..., 4, :, :, :]
    velocity = momenta / density[..., None, :, :, :]
    pressure = (GAMMA - 1.0) * (energy - 0.5 * lax.optimization_barrier(jnp.sum(momenta * velocity, axis=-4)))
    sound = jnp.sqrt(GAMMA * pressure / density)
    return (density, momenta, energy, velocity, pressure, sound)

def wave_bound(blocks):
    density, momenta, energy, velocity, pressure, sound = primitives(blocks)
    return lax.optimization_barrier(jnp.sum(jnp.abs(velocity), axis=-4)) + 3.0 * sound

def euler_flux(blocks, normal_axis):
    density, momenta, energy, velocity, pressure, sound = primitives(blocks)
    normal = velocity[..., normal_axis, :, :, :]
    parts = [momenta[..., normal_axis, :, :, :]]
    for compon in range(3):
        term = momenta[..., compon, :, :, :] * normal
        if compon == normal_axis:
            term = term + pressure
        parts.append(term)
    parts.append((energy + pressure) * normal)
    return (jnp.stack(parts, axis=-4), jnp.abs(normal) + sound)

def rusanov(left, right, normal_axis):
    flux_left, speed_left = euler_flux(left, normal_axis)
    flux_right, speed_right = euler_flux(right, normal_axis)
    speed = jnp.maximum(speed_left, speed_right)
    return 0.5 * (flux_left + flux_right) - 0.5 * speed[..., None, :, :, :] * (right - left)

def divergence(blocks, ghosts):
    extended = jnp.concatenate([ghosts[0][..., None, :, :], blocks, ghosts[1][..., None, :, :]], axis=-3)
    flux = rusanov(extended[..., :-1, :, :], extended[..., 1:, :, :], 0)
    total = flux[..., 1:, :, :] - flux[..., :-1, :, :]
    extended = jnp.concatenate([ghosts[2][..., :, None, :], blocks, ghosts[3][..., :, None, :]], axis=-2)
    flux = rusanov(extended[..., :, :-1, :], extended[..., :, 1:, :], 1)
    total = total + (flux[..., :, 1:, :] - flux[..., :, :-1, :])
    extended = jnp.concatenate([ghosts[4][..., :, :, None], blocks, ghosts[5][..., :, :, None]], axis=-1)
    flux = rusanov(extended[..., :, :, :-1], extended[..., :, :, 1:], 2)
    total = total + (flux[..., :, :, 1:] - flux[..., :, :, :-1])
    return total

def reference(state, patch_count, neighbour_table, send_table, ghost_table):
    slots_total = RANGES * SLOTS
    blocks_all = state.reshape(SLABS, slots_total, VARS, EDGE, EDGE, EDGE)
    slot_ids = jnp.arange(slots_total, dtype=jnp.int32)
    valid = slot_ids % SLOTS < patch_count[slot_ids // SLOTS]
    speeds = wave_bound(blocks_all)
    top_speed = jnp.max(jnp.where(valid[None, :, None, None, None], speeds, jnp.float32(0.0)))
    step_size = COURANT / top_speed
    face_count = slots_total * 4
    positions = jnp.arange(face_count, dtype=jnp.int32)
    home = (positions // (SLOTS * 4)).astype(jnp.int32)
    directions = positions % 4
    opposite = directions + 1 - 2 * (directions % 2)
    neighbours = neighbour_table.reshape(face_count)
    is_local = (neighbours >= 0) & (neighbours // SLOTS == home)
    local_index = jnp.where(is_local, jnp.maximum(neighbours, 0) * 4 + opposite, positions).astype(jnp.int32)
    ghost_flat = ghost_table.reshape(face_count)
    is_remote = ghost_flat >= 0
    safe_ghost = jnp.maximum(ghost_flat, 0)
    sender = (safe_ghost // MSG_SLOTS).astype(jnp.int32)
    message_slot = (safe_ghost % MSG_SLOTS).astype(jnp.int32)
    entry = send_table[sender, home, message_slot]
    remote_index = (sender * (SLOTS * 4) + jnp.maximum(entry, 0)).astype(jnp.int32)
    lower_all = jnp.concatenate([face_layer(blocks_all[:1], 4), face_layer(blocks_all[:-1], 5)], axis=0)
    upper_all = jnp.concatenate([face_layer(blocks_all[1:], 4), face_layer(blocks_all[-1:], 5)], axis=0)

    def one_slab(inputs):
        blocks, lower, upper = inputs
        faces = jnp.stack([face_layer(blocks, direction) for direction in range(4)], axis=1)
        faces = faces.reshape(face_count, VARS, EDGE, EDGE)
        local_faces = jnp.take(faces, local_index, axis=0)
        remote_faces = jnp.take(faces, remote_index, axis=0)
        remote_faces = jnp.where((entry >= 0)[:, None, None, None], remote_faces, jnp.float32(0.0))
        chosen = jnp.where(is_remote[:, None, None, None], remote_faces, local_faces)
        lateral = chosen.reshape(slots_total, 4, VARS, EDGE, EDGE)
        ghosts = [lateral[:, direction] for direction in range(4)]
        ghosts.append(lower)
        ghosts.append(upper)
        change = divergence(blocks, ghosts)
        result = jnp.where(valid[:, None, None, None, None], blocks - step_size * change, jnp.float32(0.0))
        return result.reshape(slots_total, VARS, CELLS)
    return lax.map(one_slab, (blocks_all, lower_all, upper_all))
```

```python
import functools

import jax
import jax.numpy as jnp
from jax import lax
from jax.experimental import pallas as pl
from jax.experimental.pallas import tpu as pltpu
from jax.sharding import PartitionSpec as P

EDGE = 8
VARS = 5
LANES = 128
GAMMA = 1.4
COURANT = 0.8
OFFSETS = (-2, -1, 1, 2)


def prims(cells):
    density, mx, my, mz, energy = cells
    inverse = 1.0 / density
    velocity = (mx * inverse, my * inverse, mz * inverse)
    kinetic = mx * velocity[0] + my * velocity[1] + mz * velocity[2]
    pressure = (GAMMA - 1.0) * (energy - 0.5 * kinetic)
    sound = jnp.sqrt(GAMMA * pressure * inverse)
    return velocity, pressure, sound


def flux_along(cells, prim, axis):
    velocity, pressure, sound = prim
    normal = velocity[axis]
    parts = [cells[1 + axis]]
    for compon in range(3):
        term = cells[1 + compon] * normal
        parts.append(term + pressure if compon == axis else term)
    parts.append((cells[4] + pressure) * normal)
    return parts, jnp.abs(normal) + sound


def kernel(ranges, slabs, slots, message, state_hbm, count_hbm, near_hbm, send_hbm, ghost_hbm, out_hbm,
           state, count, near, send, ghost, faces, rolled, outbox, inbox, vertical, above, below,
           ghosts, top_out, top_in, slab_out, slab_in, result,
           load_sem, table_sem, face_send, face_recv, vert_send, vert_recv,
           top_send, top_recv, slab_send, slab_recv, store_sem):
    me = lax.axis_index("morton")
    slab = lax.axis_index("group")
    tiles = state.shape[2] // LANES

    barrier = pltpu.get_barrier_semaphore()
    for step in range(1, slabs):
        pl.semaphore_signal(barrier, inc=1, device_id={"group": lax.rem(slab + step, slabs)},
                            device_id_type=pl.DeviceIdType.MESH)
    for step in range(1, ranges):
        pl.semaphore_signal(barrier, inc=1, device_id={"morton": lax.rem(me + step, ranges)},
                            device_id_type=pl.DeviceIdType.MESH)

    loads = [
        pltpu.make_async_copy(state_hbm, state, load_sem)
    ]
    tables = [
        pltpu.make_async_copy(source, target, table_sem.at[i])
        for i, (source, target) in enumerate(
            ((count_hbm, count), (near_hbm, near), (send_hbm, send), (ghost_hbm, ghost)))
    ]
    for copy in loads + tables:
        copy.start()

    lane = lax.broadcasted_iota(jnp.int32, (slots, LANES), 1)
    low_half = lane < LANES // 2
    pos_x, pos_y, pos_z = lane // 64, lane // 8 % 8, lane % 8
    sub = lax.broadcasted_iota(jnp.int32, (slots, LANES), 0)

    def permuted(value, index):
        return jnp.take_along_axis(value, index, axis=1, mode="promise_in_bounds")

    for copy in loads:
        copy.wait()
    cells = [
        [state[v, :, pl.ds(c * LANES, LANES)] for v in range(VARS)]
        for c in range(tiles)
    ]
    prim = [prims(cells[c]) for c in range(tiles)]
    tables[0].wait()
    valid = sub < count[0]
    top = None
    for velocity, pressure, sound in prim:
        bound = jnp.abs(velocity[0]) + jnp.abs(velocity[1]) + jnp.abs(velocity[2]) + 3.0 * sound
        bound = jnp.where(valid, bound, 0.0)
        top = bound if top is None else jnp.maximum(top, bound)
    top = jnp.max(top, axis=0, keepdims=True)
    top_out[...] = top

    take_y = lane // 8 % 2 * 64 + lane // 64 * 56 + lane % 8
    take_z = lane // 8 % 2 * 64 + lane % 8 * 8 + lane // 64 * 7
    piece = lane % 64 // 16

    def compact(v, index):
        found = permuted(cells[0][v], index)
        for c in range(1, tiles):
            found = jnp.where(piece == c, permuted(cells[c][v], index), found)
        return found

    own = [
        [jnp.where(low_half, cells[0][v], cells[tiles - 1][v]) for v in range(VARS)],
        [compact(v, take_y) for v in range(VARS)],
        [compact(v, take_z) for v in range(VARS)],
    ]
    face_rows = faces.reshape(2 * slots * 8, LANES)
    rolled_rows = rolled.reshape(2 * slots * 8, LANES)
    zero = jnp.zeros((slots, LANES), jnp.float32)
    for p in range(2):
        for v in range(8):
            value = own[p][v] if v < VARS else zero
            face_rows[pl.ds(p * slots * 8 + v, slots, stride=8), :] = value
            rolled_rows[pl.ds(p * slots * 8 + v, slots, stride=8), :] = (
                pltpu.roll(value, 64, 1) if v < VARS else zero)
    for v in range(VARS):
        vertical[v] = own[2][v]

    tables[2].wait()
    tile_low = lax.broadcasted_iota(jnp.int32, (8, LANES), 1) < LANES // 2
    for o, offset in enumerate(OFFSETS):
        target = lax.rem(me + offset + ranges, ranges)
        for t in range(message):
            entry = send[t, 0, target]
            safe = jnp.maximum(entry, 0)
            face = safe % 4
            index = face // 2 * slots + safe // 4
            straight, turned = faces[index], rolled[index]
            picked = jnp.where(tile_low == (face % 2 == 0), straight, turned)
            outbox[o, t] = jnp.where(entry >= 0, picked, 0.0)

    pl.semaphore_wait(barrier, ranges - 1 + slabs - 1)

    def remote(source, target, send_at, recv_at, device):
        copy = pltpu.make_async_remote_copy(
            src_ref=source, dst_ref=target, send_sem=send_at, recv_sem=recv_at,
            device_id=device, device_id_type=pl.DeviceIdType.MESH)
        copy.start()
        return copy

    top_copies = [
        remote(top_out, top_in.at[step - 1], top_send.at[step - 1], top_recv.at[step - 1],
               {"morton": lax.rem(me + step, ranges)})
        for step in range(1, ranges)
    ]
    face_copies = [
        remote(outbox.at[o], inbox.at[len(OFFSETS) - 1 - o], face_send.at[o], face_recv.at[len(OFFSETS) - 1 - o],
               {"morton": lax.rem(me + offset + ranges, ranges)})
        for o, offset in enumerate(OFFSETS)
    ]
    vert_copies = [
        remote(vertical, below, vert_send.at[0], vert_recv.at[0], {"group": lax.rem(slab + 1, slabs)}),
        remote(vertical, above, vert_send.at[1], vert_recv.at[1], {"group": lax.rem(slab + slabs - 1, slabs)}),
    ]

    def shift_up(values, axis):
        if axis == 0:
            turned = [pltpu.roll(value, 64, 1) for value in values]
            return [jnp.where(low_half, turned[max(c - 1, 0)], turned[c]) for c in range(tiles)]
        return [pltpu.roll(value, 8 if axis == 1 else 1, 1) for value in values]

    def shift_down(values, axis):
        if axis == 0:
            turned = [pltpu.roll(value, 64, 1) for value in values]
            return [jnp.where(low_half, turned[c], turned[min(c + 1, tiles - 1)]) for c in range(tiles)]
        return [pltpu.roll(value, LANES - (8 if axis == 1 else 1), 1) for value in values]

    first, last = [], []
    for axis in range(3):
        if axis == 0:
            first.append([low_half if c == 0 else None for c in range(tiles)])
            last.append([~low_half if c == tiles - 1 else None for c in range(tiles)])
        else:
            position = pos_y if axis == 1 else pos_z
            first.append([position == 0] * tiles)
            last.append([position == EDGE - 1] * tiles)

    change = [[None] * VARS for c in range(tiles)]
    for axis in range(3):
        flux = [flux_along(cells[c], prim[c], axis) for c in range(tiles)]
        speed = [flux[c][1] for c in range(tiles)]
        speed_left = shift_up(speed, axis)
        half_speed = [0.5 * jnp.maximum(speed[c], speed_left[c]) for c in range(tiles)]
        for v in range(VARS):
            here = [cells[c][v] for c in range(tiles)]
            here_flux = [flux[c][0][v] for c in range(tiles)]
            left = shift_up(here, axis)
            left_flux = shift_up(here_flux, axis)
            across = [
                0.5 * (left_flux[c] + here_flux[c]) - half_speed[c] * (here[c] - left[c])
                for c in range(tiles)
            ]
            across = [
                across[c] if first[axis][c] is None else jnp.where(first[axis][c], 0.0, across[c])
                for c in range(tiles)
            ]
            upper = shift_down(across, axis)
            for c in range(tiles):
                if last[axis][c] is not None:
                    upper[c] = jnp.where(last[axis][c], 0.0, upper[c])
                term = upper[c] - across[c]
                change[c][v] = term if change[c][v] is None else change[c][v] + term

    own_flux = [flux_along(own[axis], prims(own[axis]), axis) for axis in range(3)]

    for copy in top_copies:
        copy.wait_recv()
    top = top_out[...]
    for step in range(1, ranges):
        top = jnp.maximum(top, top_in[step - 1])
    slab_out[...] = top
    slab_copies = [
        remote(slab_out, slab_in.at[step - 1], slab_send.at[step - 1], slab_recv.at[step - 1],
               {"group": lax.rem(slab + step, slabs)})
        for step in range(1, slabs)
    ]

    tables[1].wait()
    tables[3].wait()
    for copy in face_copies + vert_copies:
        copy.wait_recv()
    for s in range(slots):
        for p in range(2):
            halves = []
            for k in (2 * p, 2 * p + 1):
                arrives = ghost[0, k, s]
                neighbour = near[0, k, s]
                inside = (neighbour >= 0) & (neighbour // slots == me)
                local = jnp.where(inside, neighbour % slots, s)
                here = jnp.where(inside, rolled[p * slots + local], faces[p * slots + s])
                safe = jnp.maximum(arrives, 0)
                distance = safe // message - me
                box = jnp.where(distance < 0, distance + 2, distance + 1)
                box = jnp.clip(box, 0, len(OFFSETS) - 1)
                there = inbox[box, safe % message]
                halves.append(jnp.where(arrives >= 0, there, here))
            ghosts[p * slots + s] = jnp.where(tile_low, halves[0], halves[1])
    ghost_rows = ghosts.reshape(2 * slots * 8, LANES)
    outer = [
        [ghost_rows[pl.ds(p * slots * 8 + v, slots, stride=8), :] for v in range(VARS)]
        for p in range(2)
    ]
    use_own = jnp.where(low_half, (slab == 0).astype(jnp.int32), (slab == slabs - 1).astype(jnp.int32)) > 0
    outer.append([
        jnp.where(use_own, own[2][v], pltpu.roll(jnp.where(low_half, above[v], below[v]), 64, 1))
        for v in range(VARS)
    ])
    sign = jnp.where(low_half, -1.0, 1.0)
    for axis in range(3):
        outer_flux, outer_speed = flux_along(outer[axis], prims(outer[axis]), axis)
        inner_flux, inner_speed = own_flux[axis]
        half_speed = 0.5 * jnp.maximum(outer_speed, inner_speed)
        for v in range(VARS):
            signed = (sign * (0.5 * (outer_flux[v] + inner_flux[v]))
                      - half_speed * (outer[axis][v] - own[axis][v]))
            for c in range(tiles):
                if axis == 0:
                    if c == 0:
                        change[c][v] = change[c][v] + jnp.where(low_half, signed, 0.0)
                    if c == tiles - 1:
                        change[c][v] = change[c][v] + jnp.where(low_half, 0.0, signed)
                else:
                    if axis == 1:
                        index = (2 * c + pos_x) * 8 + pos_z + jnp.where(pos_y >= 4, 64, 0)
                    else:
                        index = (2 * c + pos_x) * 8 + pos_y + jnp.where(pos_z >= 4, 64, 0)
                    edge = first[axis][c] | last[axis][c]
                    change[c][v] = change[c][v] + jnp.where(edge, permuted(signed, index), 0.0)

    for copy in slab_copies:
        copy.wait_recv()
    for step in range(1, slabs):
        top = jnp.maximum(top, slab_in[step - 1])
    step_size = COURANT / jnp.max(top, axis=1, keepdims=True)
    for c in range(tiles):
        for v in range(VARS):
            value = jnp.where(valid, cells[c][v] - step_size * change[c][v], 0.0)
            result[v, :, pl.ds(c * LANES, LANES)] = value
    stores = [pltpu.make_async_copy(result, out_hbm, store_sem)]
    stores[0].start()
    for copy in top_copies + face_copies + vert_copies + slab_copies:
        copy.wait_send()
    for copy in stores:
        copy.wait()


def solution(mesh):
    ranges, slabs = mesh.shape["morton"], mesh.shape["group"]

    def per_device(state, patch_count, neighbour_table, send_table, ghost_table):
        _, slots, variables, count_cells = state.shape
        message = send_table.shape[2]
        tiles = count_cells // LANES
        f32 = jnp.float32
        vmem, smem, dma = pltpu.VMEM, pltpu.SMEM, pltpu.SemaphoreType.DMA
        state = jnp.transpose(state[0], (1, 0, 2))
        neighbour_table = jnp.transpose(neighbour_table, (0, 2, 1))
        send_table = jnp.transpose(send_table, (2, 0, 1))
        ghost_table = jnp.transpose(ghost_table, (0, 2, 1))
        out = pl.pallas_call(
            functools.partial(kernel, ranges, slabs, slots, message),
            out_shape=jax.ShapeDtypeStruct(state.shape, f32),
            in_specs=[pl.BlockSpec(memory_space=pl.ANY)] * 5,
            out_specs=pl.BlockSpec(memory_space=pl.ANY),
            scratch_shapes=[
                vmem(state.shape, f32),
                smem(patch_count.shape, jnp.int32),
                smem(neighbour_table.shape, jnp.int32),
                smem(send_table.shape, jnp.int32),
                smem(ghost_table.shape, jnp.int32),
                vmem((2 * slots, 8, LANES), f32),
                vmem((2 * slots, 8, LANES), f32),
                vmem((len(OFFSETS), message, 8, LANES), f32),
                vmem((len(OFFSETS), message, 8, LANES), f32),
                vmem((VARS, slots, LANES), f32),
                vmem((VARS, slots, LANES), f32),
                vmem((VARS, slots, LANES), f32),
                vmem((2 * slots, 8, LANES), f32),
                vmem((1, LANES), f32),
                vmem((ranges - 1, 1, LANES), f32),
                vmem((1, LANES), f32),
                vmem((slabs - 1, 1, LANES), f32),
                vmem(state.shape, f32),
                dma,
                dma((4,)),
                dma((len(OFFSETS),)),
                dma((len(OFFSETS),)),
                dma((2,)),
                dma((2,)),
                dma((ranges - 1,)),
                dma((ranges - 1,)),
                dma((slabs - 1,)),
                dma((slabs - 1,)),
                dma,
            ],
            compiler_params=pltpu.CompilerParams(collective_id=0, has_side_effects=True),
        )(state, patch_count, neighbour_table, send_table, ghost_table)
        return jnp.transpose(out, (1, 0, 2))[None]

    placed = (
        P("group", "morton", None, None),
        P("morton"),
        P("morton", None, None),
        P("morton", None, None),
        P("morton", None, None),
    )
    return jax.shard_map(
        per_device,
        mesh=mesh,
        in_specs=placed,
        out_specs=P("group", "morton", None, None),
        check_vma=False,
    )
```

```python
import functools

import jax
import jax.numpy as jnp
from jax import lax
from jax.experimental import pallas as pl
from jax.experimental.pallas import tpu as pltpu
from jax.sharding import PartitionSpec as P

EDGE = 8
VARS = 5
LANES = 128
GAMMA = 1.4
COURANT = 0.8
OFFSETS = (-2, -1, 1, 2)


def prims(cells):
    density, mx, my, mz, energy = cells
    inverse = 1.0 / density
    velocity = (mx * inverse, my * inverse, mz * inverse)
    kinetic = mx * velocity[0] + my * velocity[1] + mz * velocity[2]
    pressure = (GAMMA - 1.0) * (energy - 0.5 * kinetic)
    sound = jnp.sqrt(GAMMA * pressure * inverse)
    return velocity, pressure, sound


def flux_along(cells, prim, axis):
    velocity, pressure, sound = prim
    normal = velocity[axis]
    parts = [cells[1 + axis]]
    for compon in range(3):
        term = cells[1 + compon] * normal
        parts.append(term + pressure if compon == axis else term)
    parts.append((cells[4] + pressure) * normal)
    return parts, jnp.abs(normal) + sound


def kernel(ranges, slabs, slots, message, state_hbm, count_hbm, near_hbm, send_hbm, ghost_hbm, out_ref,
           state, count, near, send, ghost, faces, rolled, outbox, inbox, vertical, above, below,
           ghosts, top_out, top_in, slab_out, slab_in,
           load_sem, table_sem, face_send, face_recv, vert_send, vert_recv,
           top_send, top_recv, slab_send, slab_recv):
    me = lax.axis_index("morton")
    slab = lax.axis_index("group")
    tiles = state.shape[2] // LANES

    barrier = pltpu.get_barrier_semaphore()
    for step in range(1, slabs):
        pl.semaphore_signal(barrier, inc=1, device_id={"group": lax.rem(slab + step, slabs)},
                            device_id_type=pl.DeviceIdType.MESH)
    for step in range(1, ranges):
        pl.semaphore_signal(barrier, inc=1, device_id={"morton": lax.rem(me + step, ranges)},
                            device_id_type=pl.DeviceIdType.MESH)

    loads = [
        pltpu.make_async_copy(state_hbm, state, load_sem)
    ]
    tables = [
        pltpu.make_async_copy(source, target, table_sem.at[i])
        for i, (source, target) in enumerate(
            ((count_hbm, count), (near_hbm, near), (send_hbm, send), (ghost_hbm, ghost)))
    ]
    for copy in loads + tables:
        copy.start()

    lane = lax.broadcasted_iota(jnp.int32, (slots, LANES), 1)
    low_half = lane < LANES // 2
    pos_x, pos_y, pos_z = lane // 64, lane // 8 % 8, lane % 8
    sub = lax.broadcasted_iota(jnp.int32, (slots, LANES), 0)

    def permuted(value, index):
        return jnp.take_along_axis(value, index, axis=1, mode="promise_in_bounds")

    for copy in loads:
        copy.wait()
    cells = [
        [state[v, :, pl.ds(c * LANES, LANES)] for v in range(VARS)]
        for c in range(tiles)
    ]
    prim = [prims(cells[c]) for c in range(tiles)]
    tables[0].wait()
    valid = sub < count[0, 0]
    top = None
    for velocity, pressure, sound in prim:
        bound = jnp.abs(velocity[0]) + jnp.abs(velocity[1]) + jnp.abs(velocity[2]) + 3.0 * sound
        bound = jnp.where(valid, bound, 0.0)
        top = bound if top is None else jnp.maximum(top, bound)
    top = jnp.max(top, axis=0, keepdims=True)
    top_out[...] = top

    take_y = lane // 8 % 2 * 64 + lane // 64 * 56 + lane % 8
    take_z = lane // 8 % 2 * 64 + lane % 8 * 8 + lane // 64 * 7
    piece = lane % 64 // 16

    def compact(v, index):
        found = permuted(cells[0][v], index)
        for c in range(1, tiles):
            found = jnp.where(piece == c, permuted(cells[c][v], index), found)
        return found

    own = [
        [jnp.where(low_half, cells[0][v], cells[tiles - 1][v]) for v in range(VARS)],
        [compact(v, take_y) for v in range(VARS)],
        [compact(v, take_z) for v in range(VARS)],
    ]
    face_rows = faces.reshape(2 * slots * 8, LANES)
    rolled_rows = rolled.reshape(2 * slots * 8, LANES)
    zero = jnp.zeros((slots, LANES), jnp.float32)
    for p in range(2):
        for v in range(8):
            value = own[p][v] if v < VARS else zero
            face_rows[pl.ds(p * slots * 8 + v, slots, stride=8), :] = value
            rolled_rows[pl.ds(p * slots * 8 + v, slots, stride=8), :] = (
                pltpu.roll(value, 64, 1) if v < VARS else zero)
    for v in range(VARS):
        vertical[v] = own[2][v]

    tables[2].wait()
    tile_low = lax.broadcasted_iota(jnp.int32, (8, LANES), 1) < LANES // 2
    for o, offset in enumerate(OFFSETS):
        target = lax.rem(me + offset + ranges, ranges)
        for t in range(message):
            entry = send[t, 0, target]
            safe = jnp.maximum(entry, 0)
            face = safe % 4
            index = face // 2 * slots + safe // 4
            straight, turned = faces[index], rolled[index]
            picked = jnp.where(tile_low == (face % 2 == 0), straight, turned)
            outbox[o, t] = jnp.where(entry >= 0, picked, 0.0)

    pl.semaphore_wait(barrier, ranges - 1 + slabs - 1)

    def remote(source, target, send_at, recv_at, device):
        copy = pltpu.make_async_remote_copy(
            src_ref=source, dst_ref=target, send_sem=send_at, recv_sem=recv_at,
            device_id=device, device_id_type=pl.DeviceIdType.MESH)
        copy.start()
        return copy

    top_copies = [
        remote(top_out, top_in.at[step - 1], top_send.at[step - 1], top_recv.at[step - 1],
               {"morton": lax.rem(me + step, ranges)})
        for step in range(1, ranges)
    ]
    face_copies = [
        remote(outbox.at[o], inbox.at[len(OFFSETS) - 1 - o], face_send.at[o], face_recv.at[len(OFFSETS) - 1 - o],
               {"morton": lax.rem(me + offset + ranges, ranges)})
        for o, offset in enumerate(OFFSETS)
    ]
    vert_copies = [
        remote(vertical, below, vert_send.at[0], vert_recv.at[0], {"group": lax.rem(slab + 1, slabs)}),
        remote(vertical, above, vert_send.at[1], vert_recv.at[1], {"group": lax.rem(slab + slabs - 1, slabs)}),
    ]

    def shift_up(values, axis):
        if axis == 0:
            turned = [pltpu.roll(value, 64, 1) for value in values]
            return [jnp.where(low_half, turned[max(c - 1, 0)], turned[c]) for c in range(tiles)]
        return [pltpu.roll(value, 8 if axis == 1 else 1, 1) for value in values]

    def shift_down(values, axis):
        if axis == 0:
            turned = [pltpu.roll(value, 64, 1) for value in values]
            return [jnp.where(low_half, turned[c], turned[min(c + 1, tiles - 1)]) for c in range(tiles)]
        return [pltpu.roll(value, LANES - (8 if axis == 1 else 1), 1) for value in values]

    first, last = [], []
    for axis in range(3):
        if axis == 0:
            first.append([low_half if c == 0 else None for c in range(tiles)])
            last.append([~low_half if c == tiles - 1 else None for c in range(tiles)])
        else:
            position = pos_y if axis == 1 else pos_z
            first.append([position == 0] * tiles)
            last.append([position == EDGE - 1] * tiles)

    change = [[None] * VARS for c in range(tiles)]
    for axis in range(3):
        flux = [flux_along(cells[c], prim[c], axis) for c in range(tiles)]
        speed = [flux[c][1] for c in range(tiles)]
        speed_left = shift_up(speed, axis)
        half_speed = [0.5 * jnp.maximum(speed[c], speed_left[c]) for c in range(tiles)]
        for v in range(VARS):
            here = [cells[c][v] for c in range(tiles)]
            here_flux = [flux[c][0][v] for c in range(tiles)]
            left = shift_up(here, axis)
            left_flux = shift_up(here_flux, axis)
            across = [
                0.5 * (left_flux[c] + here_flux[c]) - half_speed[c] * (here[c] - left[c])
                for c in range(tiles)
            ]
            across = [
                across[c] if first[axis][c] is None else jnp.where(first[axis][c], 0.0, across[c])
                for c in range(tiles)
            ]
            upper = shift_down(across, axis)
            for c in range(tiles):
                if last[axis][c] is not None:
                    upper[c] = jnp.where(last[axis][c], 0.0, upper[c])
                term = upper[c] - across[c]
                change[c][v] = term if change[c][v] is None else change[c][v] + term

    own_flux = [flux_along(own[axis], prims(own[axis]), axis) for axis in range(3)]

    for copy in top_copies:
        copy.wait_recv()
    top = top_out[...]
    for step in range(1, ranges):
        top = jnp.maximum(top, top_in[step - 1])
    slab_out[...] = top
    slab_copies = [
        remote(slab_out, slab_in.at[step - 1], slab_send.at[step - 1], slab_recv.at[step - 1],
               {"group": lax.rem(slab + step, slabs)})
        for step in range(1, slabs)
    ]

    tables[1].wait()
    tables[3].wait()
    for copy in face_copies + vert_copies:
        copy.wait_recv()
    for s in range(slots):
        for p in range(2):
            halves = []
            for k in (2 * p, 2 * p + 1):
                arrives = ghost[0, k, s]
                neighbour = near[0, k, s]
                inside = (neighbour >= 0) & (neighbour // slots == me)
                local = jnp.where(inside, neighbour % slots, s)
                here = jnp.where(inside, rolled[p * slots + local], faces[p * slots + s])
                safe = jnp.maximum(arrives, 0)
                distance = safe // message - me
                box = jnp.where(distance < 0, distance + 2, distance + 1)
                box = jnp.clip(box, 0, len(OFFSETS) - 1)
                there = inbox[box, safe % message]
                halves.append(jnp.where(arrives >= 0, there, here))
            ghosts[p * slots + s] = jnp.where(tile_low, halves[0], halves[1])
    ghost_rows = ghosts.reshape(2 * slots * 8, LANES)
    outer = [
        [ghost_rows[pl.ds(p * slots * 8 + v, slots, stride=8), :] for v in range(VARS)]
        for p in range(2)
    ]
    use_own = jnp.where(low_half, (slab == 0).astype(jnp.int32), (slab == slabs - 1).astype(jnp.int32)) > 0
    outer.append([
        jnp.where(use_own, own[2][v], pltpu.roll(jnp.where(low_half, above[v], below[v]), 64, 1))
        for v in range(VARS)
    ])
    sign = jnp.where(low_half, -1.0, 1.0)
    for axis in range(3):
        outer_flux, outer_speed = flux_along(outer[axis], prims(outer[axis]), axis)
        inner_flux, inner_speed = own_flux[axis]
        half_speed = 0.5 * jnp.maximum(outer_speed, inner_speed)
        for v in range(VARS):
            signed = (sign * (0.5 * (outer_flux[v] + inner_flux[v]))
                      - half_speed * (outer[axis][v] - own[axis][v]))
            for c in range(tiles):
                if axis == 0:
                    if c == 0:
                        change[c][v] = change[c][v] + jnp.where(low_half, signed, 0.0)
                    if c == tiles - 1:
                        change[c][v] = change[c][v] + jnp.where(low_half, 0.0, signed)
                else:
                    if axis == 1:
                        index = (2 * c + pos_x) * 8 + pos_z + jnp.where(pos_y >= 4, 64, 0)
                    else:
                        index = (2 * c + pos_x) * 8 + pos_y + jnp.where(pos_z >= 4, 64, 0)
                    edge = first[axis][c] | last[axis][c]
                    change[c][v] = change[c][v] + jnp.where(edge, permuted(signed, index), 0.0)

    for copy in slab_copies:
        copy.wait_recv()
    for step in range(1, slabs):
        top = jnp.maximum(top, slab_in[step - 1])
    step_size = COURANT / jnp.max(top, axis=1, keepdims=True)
    for c in range(tiles):
        for v in range(VARS):
            value = jnp.where(valid, cells[c][v] - step_size * change[c][v], 0.0)
            out_ref[v, :, pl.ds(c * LANES, LANES)] = value
    for copy in top_copies + face_copies + vert_copies + slab_copies:
        copy.wait_send()


def solution(mesh):
    ranges, slabs = mesh.shape["morton"], mesh.shape["group"]

    def per_device(state, patch_count, neighbour_table, send_table, ghost_table):
        _, slots, variables, count_cells = state.shape
        message = send_table.shape[2]
        tiles = count_cells // LANES
        f32 = jnp.float32
        vmem, smem, dma = pltpu.VMEM, pltpu.SMEM, pltpu.SemaphoreType.DMA
        state = jnp.transpose(state[0], (1, 0, 2))
        patch_count = patch_count.reshape(1, 1)
        neighbour_table = jnp.transpose(neighbour_table, (0, 2, 1))
        send_table = jnp.transpose(send_table, (2, 0, 1))
        ghost_table = jnp.transpose(ghost_table, (0, 2, 1))
        out = pl.pallas_call(
            functools.partial(kernel, ranges, slabs, slots, message),
            out_shape=pltpu.VMEM(state.shape, f32),
            in_specs=[pl.BlockSpec(memory_space=pltpu.HBM)] * 5,
            out_specs=pl.BlockSpec(memory_space=pltpu.VMEM),
            scratch_shapes=[
                vmem(state.shape, f32),
                smem(patch_count.shape, jnp.int32),
                smem(neighbour_table.shape, jnp.int32),
                smem(send_table.shape, jnp.int32),
                smem(ghost_table.shape, jnp.int32),
                vmem((2 * slots, 8, LANES), f32),
                vmem((2 * slots, 8, LANES), f32),
                vmem((len(OFFSETS), message, 8, LANES), f32),
                vmem((len(OFFSETS), message, 8, LANES), f32),
                vmem((VARS, slots, LANES), f32),
                vmem((VARS, slots, LANES), f32),
                vmem((VARS, slots, LANES), f32),
                vmem((2 * slots, 8, LANES), f32),
                vmem((1, LANES), f32),
                vmem((ranges - 1, 1, LANES), f32),
                vmem((1, LANES), f32),
                vmem((slabs - 1, 1, LANES), f32),
                dma,
                dma((4,)),
                dma((len(OFFSETS),)),
                dma((len(OFFSETS),)),
                dma((2,)),
                dma((2,)),
                dma((ranges - 1,)),
                dma((ranges - 1,)),
                dma((slabs - 1,)),
                dma((slabs - 1,)),
            ],
            compiler_params=pltpu.CompilerParams(collective_id=0, has_side_effects=True),
        )(state, patch_count, neighbour_table, send_table, ghost_table)
        return jnp.transpose(out, (1, 0, 2))[None]

    placed = (
        P("group", "morton", None, None),
        P("morton"),
        P("morton", None, None),
        P("morton", None, None),
        P("morton", None, None),
    )
    return jax.shard_map(
        per_device,
        mesh=mesh,
        in_specs=placed,
        out_specs=P("group", "morton", None, None),
        check_vma=False,
    )
```

```python
import functools

import jax
import jax.numpy as jnp
from jax import lax
from jax.experimental import pallas as pl
from jax.experimental.pallas import tpu as pltpu
from jax.sharding import PartitionSpec as P

EDGE = 8
VARS = 5
LANES = 128
GAMMA = 1.4
COURANT = 0.8
REACH = 2
OFFSETS = (-2, 2, -1, 1)


def prims(cells):
    density, mx, my, mz, energy = cells
    inverse = 1.0 / density
    velocity = (mx * inverse, my * inverse, mz * inverse)
    kinetic = mx * velocity[0] + my * velocity[1] + mz * velocity[2]
    pressure = (GAMMA - 1.0) * (energy - 0.5 * kinetic)
    sound = jnp.sqrt(GAMMA * pressure * inverse)
    return velocity, pressure, sound


def flux_along(cells, prim, axis):
    velocity, pressure, sound = prim
    normal = velocity[axis]
    parts = [cells[1 + axis]]
    for compon in range(3):
        term = cells[1 + compon] * normal
        parts.append(term + pressure if compon == axis else term)
    parts.append((cells[4] + pressure) * normal)
    return parts, jnp.abs(normal) + sound


def kernel(ranges, slabs, phases, slots, message, state_hbm, count_hbm, near_hbm, send_hbm, ghost_hbm, out_ref,
           state, count, near, send, ghost, faces, rolled, outbox, inbox, vertical, above, below,
           ghosts, top_out, top_in,
           load_sem, table_sem, face_send, face_recv, vert_send, vert_recv,
           top_send, top_recv):
    me = lax.axis_index("morton")
    slab = lax.axis_index("group")
    tiles = state.shape[2] // LANES

    barrier = pltpu.get_barrier_semaphore()
    def device(step):
        return {"group": lax.rem(slab + step[0], slabs), "morton": lax.rem(me + step[1], ranges)}

    for phase in phases:
        for step in phase:
            pl.semaphore_signal(barrier, inc=1, device_id=device(step), device_id_type=pl.DeviceIdType.MESH)

    loads = [
        pltpu.make_async_copy(state_hbm, state, load_sem)
    ]
    tables = [
        pltpu.make_async_copy(source, target, table_sem.at[i])
        for i, (source, target) in enumerate(
            ((count_hbm, count), (near_hbm, near), (send_hbm, send), (ghost_hbm, ghost)))
    ]
    for copy in tables + loads:
        copy.start()

    lane = lax.broadcasted_iota(jnp.int32, (slots, LANES), 1)
    low_half = lane < LANES // 2
    pos_x, pos_y, pos_z = lane // 64, lane // 8 % 8, lane % 8
    sub = lax.broadcasted_iota(jnp.int32, (slots, LANES), 0)

    def permuted(value, index):
        return jnp.take_along_axis(value, index, axis=1, mode="promise_in_bounds")

    for copy in loads:
        copy.wait()
    cells = [
        [state[v, :, pl.ds(c * LANES, LANES)] for v in range(VARS)]
        for c in range(tiles)
    ]
    prim = [prims(cells[c]) for c in range(tiles)]
    tables[0].wait()
    valid = sub < count[0, 0]
    top = None
    for velocity, pressure, sound in prim:
        bound = jnp.abs(velocity[0]) + jnp.abs(velocity[1]) + jnp.abs(velocity[2]) + 3.0 * sound
        bound = jnp.where(valid, bound, 0.0)
        top = bound if top is None else jnp.maximum(top, bound)
    top = jnp.max(top, axis=0, keepdims=True)
    top_out[0] = top

    pl.semaphore_wait(barrier, sum(len(phase) for phase in phases))

    def remote(source, target, send_at, recv_at, device):
        copy = pltpu.make_async_remote_copy(
            src_ref=source, dst_ref=target, send_sem=send_at, recv_sem=recv_at,
            device_id=device, device_id_type=pl.DeviceIdType.MESH)
        copy.start()
        return copy

    def exchange(source, number):
        first_slot = sum(len(phase) for phase in phases[:number])
        return [
            (remote(source, top_in.at[n], top_send.at[n], top_recv.at[n], device(step)), n)
            for n, step in enumerate(phases[number], first_slot)
        ]

    def gathered(top, copies):
        for copy, n in copies:
            copy.wait_recv()
        for copy, n in copies:
            top = jnp.maximum(top, top_in[n])
        return top

    top_copies = exchange(top_out.at[0], 0)

    take_y = lane // 8 % 2 * 64 + lane // 64 * 56 + lane % 8
    take_z = lane // 8 % 2 * 64 + lane % 8 * 8 + lane // 64 * 7
    piece = lane % 64 // 16

    def compact(v, index):
        found = permuted(cells[0][v], index)
        for c in range(1, tiles):
            found = jnp.where(piece == c, permuted(cells[c][v], index), found)
        return found

    own = [
        [jnp.where(low_half, cells[0][v], cells[tiles - 1][v]) for v in range(VARS)],
        [compact(v, take_y) for v in range(VARS)],
        [compact(v, take_z) for v in range(VARS)],
    ]
    face_rows = faces.reshape(2 * slots * 8, LANES)
    rolled_rows = rolled.reshape(2 * slots * 8, LANES)
    for p in range(2):
        for v in range(VARS):
            value = own[p][v]
            face_rows[pl.ds(p * slots * 8 + v, slots, stride=8), :] = value
            rolled_rows[pl.ds(p * slots * 8 + v, slots, stride=8), :] = pltpu.roll(value, 64, 1)
    turned = [pltpu.roll(value, 64, 1) for value in own[2]]
    for v in range(0, VARS, 2):
        last_one = v + 1 == VARS
        vertical[0, v // 2] = turned[v] if last_one else jnp.where(low_half, turned[v], own[2][v + 1])
        vertical[1, v // 2] = own[2][v] if last_one else jnp.where(low_half, own[2][v], turned[v + 1])

    tables[2].wait()
    tile_low = lax.broadcasted_iota(jnp.int32, (8, LANES), 1) < LANES // 2
    for o, offset in enumerate(OFFSETS):
        target = jnp.clip(me + offset, 0, ranges - 1)
        for t in range(message):
            entry = send[t, 0, target]
            safe = jnp.maximum(entry, 0)
            face = safe & 3
            index = (face >> 1) * slots + (safe >> 2)
            straight, turned = faces[index], rolled[index]
            picked = jnp.where(tile_low == ((face & 1) == 0), straight, turned)
            outbox[o, t] = jnp.where(entry >= 0, picked, 0.0)

    def guarded(source, target, send_at, recv_at, device, sends, receives):
        copy = pltpu.make_async_remote_copy(
            src_ref=source, dst_ref=target, send_sem=send_at, recv_sem=recv_at,
            device_id=device, device_id_type=pl.DeviceIdType.MESH)
        pl.when(sends)(copy.start)
        return copy, sends, receives

    edge_copies = [
        guarded(vertical.at[0], below, vert_send.at[0], vert_recv.at[0],
                {"group": jnp.minimum(slab + 1, slabs - 1)}, slab < slabs - 1, slab > 0),
        guarded(vertical.at[1], above, vert_send.at[1], vert_recv.at[1],
                {"group": jnp.maximum(slab - 1, 0)}, slab > 0, slab < slabs - 1),
    ]
    for o, offset in enumerate(OFFSETS):
        sends = (me + offset >= 0) & (me + offset < ranges)
        receives = (me - offset >= 0) & (me - offset < ranges)
        edge_copies.append(guarded(
            outbox.at[o, :, pl.ds(0, VARS), :],
            inbox.at[pl.ds((REACH - offset) * message, message), pl.ds(0, VARS), :],
            face_send.at[o], face_recv.at[o],
            {"morton": jnp.clip(me + offset, 0, ranges - 1)}, sends, receives))

    tables[1].wait()
    tables[3].wait()
    for s in range(slots):
        for p in range(2):
            halves = []
            for k in (2 * p, 2 * p + 1):
                local = near[0, k, s] - me * slots
                inside = (local >= 0) & (local < slots)
                local = jnp.clip(local, 0, slots - 1)
                halves.append(jnp.where(inside, rolled[p * slots + local], faces[p * slots + s]))
            ghosts[p * slots + s] = jnp.where(tile_low, halves[0], halves[1])

    def shift_up(values, axis):
        if axis == 0:
            turned = [pltpu.roll(value, 64, 1) for value in values]
            return [jnp.where(low_half, turned[max(c - 1, 0)], turned[c]) for c in range(tiles)]
        return [pltpu.roll(value, 8 if axis == 1 else 1, 1) for value in values]

    def shift_down(values, axis):
        if axis == 0:
            turned = [pltpu.roll(value, 64, 1) for value in values]
            return [jnp.where(low_half, turned[c], turned[min(c + 1, tiles - 1)]) for c in range(tiles)]
        return [pltpu.roll(value, LANES - (8 if axis == 1 else 1), 1) for value in values]

    first, last = [], []
    for axis in range(3):
        if axis == 0:
            first.append([low_half if c == 0 else None for c in range(tiles)])
            last.append([~low_half if c == tiles - 1 else None for c in range(tiles)])
        else:
            position = pos_y if axis == 1 else pos_z
            first.append([position == 0] * tiles)
            last.append([position == EDGE - 1] * tiles)

    change = [[None] * VARS for c in range(tiles)]
    for axis in range(3):
        flux = [flux_along(cells[c], prim[c], axis) for c in range(tiles)]
        speed = [flux[c][1] for c in range(tiles)]
        speed_left = shift_up(speed, axis)
        half_speed = [0.5 * jnp.maximum(speed[c], speed_left[c]) for c in range(tiles)]
        for v in range(VARS):
            here = [cells[c][v] for c in range(tiles)]
            here_flux = [flux[c][0][v] for c in range(tiles)]
            left = shift_up(here, axis)
            left_flux = shift_up(here_flux, axis)
            across = [
                0.5 * (left_flux[c] + here_flux[c]) - half_speed[c] * (here[c] - left[c])
                for c in range(tiles)
            ]
            across = [
                across[c] if first[axis][c] is None else jnp.where(first[axis][c], 0.0, across[c])
                for c in range(tiles)
            ]
            upper = shift_down(across, axis)
            for c in range(tiles):
                if last[axis][c] is not None:
                    upper[c] = jnp.where(last[axis][c], 0.0, upper[c])
                term = upper[c] - across[c]
                change[c][v] = term if change[c][v] is None else change[c][v] + term

    own_flux = [flux_along(own[axis], prims(own[axis]), axis) for axis in range(3)]

    if len(phases) > 1:
        top = gathered(top_out[0], top_copies)
        top_out[1] = top
        slab_copies = exchange(top_out.at[1], 1)
    else:
        top, slab_copies = top_out[0], []

    for copy, sends, receives in edge_copies:
        pl.when(receives)(copy.wait_recv)
    for s in range(slots):
        for p in range(2):
            halves = []
            for k in (2 * p, 2 * p + 1):
                arrives = ghost[0, k, s]
                place = jnp.clip(arrives - (me - REACH) * message, 0, (2 * REACH + 1) * message - 1)
                half = tile_low if k % 2 == 0 else ~tile_low
                halves.append((half & (arrives >= 0), inbox[place]))
            value = ghosts[p * slots + s]
            for mask, there in halves:
                value = jnp.where(mask, there, value)
            ghosts[p * slots + s] = value
    ghost_rows = ghosts.reshape(2 * slots * 8, LANES)
    outer = [
        [ghost_rows[pl.ds(p * slots * 8 + v, slots, stride=8), :] for v in range(VARS)]
        for p in range(2)
    ]
    use_own = jnp.where(low_half, (slab == 0).astype(jnp.int32), (slab == slabs - 1).astype(jnp.int32)) > 0
    outer.append([])
    for v in range(VARS):
        low, high = below[v // 2], above[v // 2]
        if v % 2 == 0:
            high = pltpu.roll(high, 64, 1)
        else:
            low = pltpu.roll(low, 64, 1)
        outer[2].append(jnp.where(use_own, own[2][v], jnp.where(low_half, low, high)))
    sign = jnp.where(low_half, -1.0, 1.0)
    for axis in range(3):
        outer_flux, outer_speed = flux_along(outer[axis], prims(outer[axis]), axis)
        inner_flux, inner_speed = own_flux[axis]
        half_speed = 0.5 * jnp.maximum(outer_speed, inner_speed)
        for v in range(VARS):
            signed = (sign * (0.5 * (outer_flux[v] + inner_flux[v]))
                      - half_speed * (outer[axis][v] - own[axis][v]))
            for c in range(tiles):
                if axis == 0:
                    if c == 0:
                        change[c][v] = change[c][v] + jnp.where(low_half, signed, 0.0)
                    if c == tiles - 1:
                        change[c][v] = change[c][v] + jnp.where(low_half, 0.0, signed)
                else:
                    if axis == 1:
                        index = (2 * c + pos_x) * 8 + pos_z + jnp.where(pos_y >= 4, 64, 0)
                    else:
                        index = (2 * c + pos_x) * 8 + pos_y + jnp.where(pos_z >= 4, 64, 0)
                    edge = first[axis][c] | last[axis][c]
                    change[c][v] = change[c][v] + jnp.where(edge, permuted(signed, index), 0.0)

    top = gathered(top, slab_copies or top_copies)
    step_size = COURANT / jnp.max(top, axis=1, keepdims=True)
    for c in range(tiles):
        for v in range(VARS):
            value = jnp.where(valid, cells[c][v] - step_size * change[c][v], 0.0)
            out_ref[v, :, pl.ds(c * LANES, LANES)] = value
    for copy, n in top_copies + slab_copies:
        copy.wait_send()
    for copy, sends, receives in edge_copies:
        pl.when(sends)(copy.wait_send)


def solution(mesh):
    ranges, slabs = mesh.shape["morton"], mesh.shape["group"]

    along_group = [(g, 0) for g in range(1, slabs)]
    along_morton = [(0, r) for r in range(1, ranges)]
    across = [(g, r) for g in range(1, slabs) for r in range(1, ranges)]
    phases = [across + along_group + along_morton] if ranges * slabs <= 64 else [along_morton, along_group]
    partners = sum(len(phase) for phase in phases)

    def per_device(state, patch_count, neighbour_table, send_table, ghost_table):
        _, slots, variables, count_cells = state.shape
        message = send_table.shape[2]
        tiles = count_cells // LANES
        f32 = jnp.float32
        vmem, smem, dma = pltpu.VMEM, pltpu.SMEM, pltpu.SemaphoreType.DMA
        state = jnp.transpose(state[0], (1, 0, 2))
        patch_count = patch_count.reshape(1, 1)
        neighbour_table = jnp.transpose(neighbour_table, (0, 2, 1))
        send_table = jnp.transpose(send_table, (2, 0, 1))
        ghost_table = jnp.transpose(ghost_table, (0, 2, 1))
        out = pl.pallas_call(
            functools.partial(kernel, ranges, slabs, phases, slots, message),
            out_shape=pltpu.VMEM(state.shape, f32),
            in_specs=[pl.BlockSpec(memory_space=pltpu.HBM)] * 5,
            out_specs=pl.BlockSpec(memory_space=pltpu.VMEM),
            scratch_shapes=[
                vmem(state.shape, f32),
                smem(patch_count.shape, jnp.int32),
                smem(neighbour_table.shape, jnp.int32),
                smem(send_table.shape, jnp.int32),
                smem(ghost_table.shape, jnp.int32),
                vmem((2 * slots, 8, LANES), f32),
                vmem((2 * slots, 8, LANES), f32),
                vmem((len(OFFSETS), message, 8, LANES), f32),
                vmem(((2 * REACH + 1) * message, 8, LANES), f32),
                vmem((2, (VARS + 1) // 2, slots, LANES), f32),
                vmem(((VARS + 1) // 2, slots, LANES), f32),
                vmem(((VARS + 1) // 2, slots, LANES), f32),
                vmem((2 * slots, 8, LANES), f32),
                vmem((2, 1, LANES), f32),
                vmem((partners, 1, LANES), f32),
                dma,
                dma((4,)),
                dma((len(OFFSETS),)),
                dma((len(OFFSETS),)),
                dma((2,)),
                dma((2,)),
                dma((partners,)),
                dma((partners,)),
            ],
            compiler_params=pltpu.CompilerParams(collective_id=0, has_side_effects=True),
        )(state, patch_count, neighbour_table, send_table, ghost_table)
        return jnp.transpose(out, (1, 0, 2))[None]

    placed = (
        P("group", "morton", None, None),
        P("morton"),
        P("morton", None, None),
        P("morton", None, None),
        P("morton", None, None),
    )
    return jax.shard_map(
        per_device,
        mesh=mesh,
        in_specs=placed,
        out_specs=P("group", "morton", None, None),
        check_vma=False,
    )
```

```python
import functools

import jax
import jax.numpy as jnp
from jax import lax
from jax.experimental import pallas as pl
from jax.experimental.pallas import tpu as pltpu
from jax.sharding import PartitionSpec as P

EDGE = 8
VARS = 5
LANES = 128
GAMMA = 1.4
COURANT = 0.8
REACH = 2
OFFSETS = (-2, 2, -1, 1)


def prims(cells):
    density, mx, my, mz, energy = cells
    inverse = 1.0 / density
    velocity = (mx * inverse, my * inverse, mz * inverse)
    kinetic = mx * velocity[0] + my * velocity[1] + mz * velocity[2]
    pressure = (GAMMA - 1.0) * (energy - 0.5 * kinetic)
    sound = jnp.sqrt(GAMMA * pressure * inverse)
    return velocity, pressure, sound


def flux_along(cells, prim, axis):
    velocity, pressure, sound = prim
    normal = velocity[axis]
    parts = [cells[1 + axis]]
    for compon in range(3):
        term = cells[1 + compon] * normal
        parts.append(term + pressure if compon == axis else term)
    parts.append((cells[4] + pressure) * normal)
    return parts, jnp.abs(normal) + sound


def flipped(index, bits):
    bit = 1
    while bit <= bits:
        if bits & bit:
            index = index + bit * (1 - 2 * (index // bit % 2))
        bit *= 2
    return index


def kernel(ranges, slabs, phases, slots, message, state_hbm, count_hbm, near_hbm, send_hbm, ghost_hbm, out_ref,
           state, count, near, send, ghost, faces, rolled, outbox, inbox, vertical, above, below,
           ghosts, top_out, top_in,
           load_sem, table_sem, face_send, face_recv, vert_send, vert_recv,
           top_send, top_recv):
    me = lax.axis_index("morton")
    slab = lax.axis_index("group")
    tiles = state.shape[2] // LANES

    barrier = pltpu.get_barrier_semaphore()
    def device(step):
        if slabs & (slabs - 1) or ranges & (ranges - 1):
            return {"group": lax.rem(slab + step[0], slabs), "morton": lax.rem(me + step[1], ranges)}
        return {"group": flipped(slab, step[0]), "morton": flipped(me, step[1])}

    for phase in phases:
        for step in phase:
            pl.semaphore_signal(barrier, inc=1, device_id=device(step), device_id_type=pl.DeviceIdType.MESH)

    loads = [
        pltpu.make_async_copy(state_hbm, state, load_sem)
    ]
    tables = [
        pltpu.make_async_copy(source, target, table_sem.at[i])
        for i, (source, target) in enumerate(
            ((count_hbm, count), (near_hbm, near), (send_hbm, send), (ghost_hbm, ghost)))
    ]
    for copy in tables + loads:
        copy.start()

    lane = lax.broadcasted_iota(jnp.int32, (slots, LANES), 1)
    low_half = lane < LANES // 2
    pos_x, pos_y, pos_z = lane // 64, lane // 8 % 8, lane % 8
    sub = lax.broadcasted_iota(jnp.int32, (slots, LANES), 0)

    def permuted(value, index):
        return jnp.take_along_axis(value, index, axis=1, mode="promise_in_bounds")

    for copy in loads:
        copy.wait()
    cells = [
        [state[v, :, pl.ds(c * LANES, LANES)] for v in range(VARS)]
        for c in range(tiles)
    ]
    prim = [prims(cells[c]) for c in range(tiles)]
    tables[0].wait()
    valid = sub < count[0, 0]
    top = None
    for velocity, pressure, sound in prim:
        bound = jnp.abs(velocity[0]) + jnp.abs(velocity[1]) + jnp.abs(velocity[2]) + 3.0 * sound
        bound = jnp.where(valid, bound, 0.0)
        top = bound if top is None else jnp.maximum(top, bound)
    top = jnp.max(top, axis=0, keepdims=True)
    top_out[0] = top

    pl.semaphore_wait(barrier, sum(len(phase) for phase in phases))

    def remote(source, target, send_at, recv_at, device):
        copy = pltpu.make_async_remote_copy(
            src_ref=source, dst_ref=target, send_sem=send_at, recv_sem=recv_at,
            device_id=device, device_id_type=pl.DeviceIdType.MESH)
        copy.start()
        return copy

    def exchange(source, number):
        first_slot = sum(len(phase) for phase in phases[:number])
        return [
            (remote(source, top_in.at[n], top_send.at[n], top_recv.at[n], device(step)), n)
            for n, step in enumerate(phases[number], first_slot)
        ]

    def gathered(top, copies):
        for copy, n in copies:
            copy.wait_recv()
        for copy, n in copies:
            top = jnp.maximum(top, top_in[n])
        return top

    top_copies = exchange(top_out.at[0], 0)

    take_y = lane // 8 % 2 * 64 + lane // 64 * 56 + lane % 8
    take_z = lane // 8 % 2 * 64 + lane % 8 * 8 + lane // 64 * 7
    piece = lane % 64 // 16

    def compact(v, index):
        found = permuted(cells[0][v], index)
        for c in range(1, tiles):
            found = jnp.where(piece == c, permuted(cells[c][v], index), found)
        return found

    own = [
        [jnp.where(low_half, cells[0][v], cells[tiles - 1][v]) for v in range(VARS)],
        [compact(v, take_y) for v in range(VARS)],
        [compact(v, take_z) for v in range(VARS)],
    ]
    face_rows = faces.reshape(2 * slots * 8, LANES)
    rolled_rows = rolled.reshape(2 * slots * 8, LANES)
    for p in range(2):
        for v in range(VARS):
            value = own[p][v]
            face_rows[pl.ds(p * slots * 8 + v, slots, stride=8), :] = value
            rolled_rows[pl.ds(p * slots * 8 + v, slots, stride=8), :] = pltpu.roll(value, 64, 1)
    turned = [pltpu.roll(value, 64, 1) for value in own[2]]
    for v in range(0, VARS, 2):
        last_one = v + 1 == VARS
        vertical[0, v // 2] = turned[v] if last_one else jnp.where(low_half, turned[v], own[2][v + 1])
        vertical[1, v // 2] = own[2][v] if last_one else jnp.where(low_half, own[2][v], turned[v + 1])

    tables[2].wait()
    tile_low = lax.broadcasted_iota(jnp.int32, (8, LANES), 1) < LANES // 2
    for o, offset in enumerate(OFFSETS):
        target = jnp.clip(me + offset, 0, ranges - 1)
        for t in range(message):
            entry = send[t, 0, target]
            safe = jnp.maximum(entry, 0)
            face = safe & 3
            index = (face >> 1) * slots + (safe >> 2)
            straight, turned = faces[index], rolled[index]
            picked = jnp.where(tile_low == ((face & 1) == 0), straight, turned)
            outbox[o, t] = jnp.where(entry >= 0, picked, 0.0)

    def guarded(source, target, send_at, recv_at, device, sends, receives):
        copy = pltpu.make_async_remote_copy(
            src_ref=source, dst_ref=target, send_sem=send_at, recv_sem=recv_at,
            device_id=device, device_id_type=pl.DeviceIdType.MESH)
        pl.when(sends)(copy.start)
        return copy, sends, receives

    edge_copies = [
        guarded(vertical.at[0], below, vert_send.at[0], vert_recv.at[0],
                {"group": jnp.minimum(slab + 1, slabs - 1)}, slab < slabs - 1, slab > 0),
        guarded(vertical.at[1], above, vert_send.at[1], vert_recv.at[1],
                {"group": jnp.maximum(slab - 1, 0)}, slab > 0, slab < slabs - 1),
    ]
    for o, offset in enumerate(OFFSETS):
        sends = (me + offset >= 0) & (me + offset < ranges)
        receives = (me - offset >= 0) & (me - offset < ranges)
        edge_copies.append(guarded(
            outbox.at[o, :, pl.ds(0, VARS), :],
            inbox.at[pl.ds((REACH - offset) * message, message), pl.ds(0, VARS), :],
            face_send.at[o], face_recv.at[o],
            {"morton": jnp.clip(me + offset, 0, ranges - 1)}, sends, receives))

    tables[1].wait()
    tables[3].wait()
    for s in range(slots):
        for p in range(2):
            halves = []
            for k in (2 * p, 2 * p + 1):
                local = near[0, k, s] - me * slots
                inside = (local >= 0) & (local < slots)
                local = jnp.clip(local, 0, slots - 1)
                halves.append(jnp.where(inside, rolled[p * slots + local], faces[p * slots + s]))
            ghosts[p * slots + s] = jnp.where(tile_low, halves[0], halves[1])

    def shift_up(values, axis):
        if axis == 0:
            turned = [pltpu.roll(value, 64, 1) for value in values]
            return [jnp.where(low_half, turned[max(c - 1, 0)], turned[c]) for c in range(tiles)]
        return [pltpu.roll(value, 8 if axis == 1 else 1, 1) for value in values]

    def shift_down(values, axis):
        if axis == 0:
            turned = [pltpu.roll(value, 64, 1) for value in values]
            return [jnp.where(low_half, turned[c], turned[min(c + 1, tiles - 1)]) for c in range(tiles)]
        return [pltpu.roll(value, LANES - (8 if axis == 1 else 1), 1) for value in values]

    first, last = [], []
    for axis in range(3):
        if axis == 0:
            first.append([low_half if c == 0 else None for c in range(tiles)])
            last.append([~low_half if c == tiles - 1 else None for c in range(tiles)])
        else:
            position = pos_y if axis == 1 else pos_z
            first.append([position == 0] * tiles)
            last.append([position == EDGE - 1] * tiles)

    change = [[None] * VARS for c in range(tiles)]
    for axis in range(3):
        flux = [flux_along(cells[c], prim[c], axis) for c in range(tiles)]
        speed = [flux[c][1] for c in range(tiles)]
        speed_left = shift_up(speed, axis)
        half_speed = [0.5 * jnp.maximum(speed[c], speed_left[c]) for c in range(tiles)]
        for v in range(VARS):
            here = [cells[c][v] for c in range(tiles)]
            here_flux = [flux[c][0][v] for c in range(tiles)]
            left = shift_up(here, axis)
            left_flux = shift_up(here_flux, axis)
            across = [
                0.5 * (left_flux[c] + here_flux[c]) - half_speed[c] * (here[c] - left[c])
                for c in range(tiles)
            ]
            across = [
                across[c] if first[axis][c] is None else jnp.where(first[axis][c], 0.0, across[c])
                for c in range(tiles)
            ]
            upper = shift_down(across, axis)
            for c in range(tiles):
                if last[axis][c] is not None:
                    upper[c] = jnp.where(last[axis][c], 0.0, upper[c])
                term = upper[c] - across[c]
                change[c][v] = term if change[c][v] is None else change[c][v] + term

    own_flux = [flux_along(own[axis], prims(own[axis]), axis) for axis in range(3)]

    if len(phases) > 1:
        top = gathered(top_out[0], top_copies)
        top_out[1] = top
        slab_copies = exchange(top_out.at[1], 1)
    else:
        top, slab_copies = top_out[0], []

    for copy, sends, receives in edge_copies:
        pl.when(receives)(copy.wait_recv)
    for s in range(slots):
        for p in range(2):
            halves = []
            for k in (2 * p, 2 * p + 1):
                arrives = ghost[0, k, s]
                place = jnp.clip(arrives - (me - REACH) * message, 0, (2 * REACH + 1) * message - 1)
                half = tile_low if k % 2 == 0 else ~tile_low
                halves.append((half & (arrives >= 0), inbox[place]))
            value = ghosts[p * slots + s]
            for mask, there in halves:
                value = jnp.where(mask, there, value)
            ghosts[p * slots + s] = value
    ghost_rows = ghosts.reshape(2 * slots * 8, LANES)
    outer = [
        [ghost_rows[pl.ds(p * slots * 8 + v, slots, stride=8), :] for v in range(VARS)]
        for p in range(2)
    ]
    use_own = jnp.where(low_half, (slab == 0).astype(jnp.int32), (slab == slabs - 1).astype(jnp.int32)) > 0
    outer.append([])
    for v in range(VARS):
        low, high = below[v // 2], above[v // 2]
        if v % 2 == 0:
            high = pltpu.roll(high, 64, 1)
        else:
            low = pltpu.roll(low, 64, 1)
        outer[2].append(jnp.where(use_own, own[2][v], jnp.where(low_half, low, high)))
    sign = jnp.where(low_half, -1.0, 1.0)
    for axis in range(3):
        outer_flux, outer_speed = flux_along(outer[axis], prims(outer[axis]), axis)
        inner_flux, inner_speed = own_flux[axis]
        half_speed = 0.5 * jnp.maximum(outer_speed, inner_speed)
        for v in range(VARS):
            signed = (sign * (0.5 * (outer_flux[v] + inner_flux[v]))
                      - half_speed * (outer[axis][v] - own[axis][v]))
            for c in range(tiles):
                if axis == 0:
                    if c == 0:
                        change[c][v] = change[c][v] + jnp.where(low_half, signed, 0.0)
                    if c == tiles - 1:
                        change[c][v] = change[c][v] + jnp.where(low_half, 0.0, signed)
                else:
                    if axis == 1:
                        index = (2 * c + pos_x) * 8 + pos_z + jnp.where(pos_y >= 4, 64, 0)
                    else:
                        index = (2 * c + pos_x) * 8 + pos_y + jnp.where(pos_z >= 4, 64, 0)
                    edge = first[axis][c] | last[axis][c]
                    change[c][v] = change[c][v] + jnp.where(edge, permuted(signed, index), 0.0)

    top = gathered(top, slab_copies or top_copies)
    step_size = COURANT / jnp.max(top, axis=1, keepdims=True)
    for c in range(tiles):
        for v in range(VARS):
            value = jnp.where(valid, cells[c][v] - step_size * change[c][v], 0.0)
            out_ref[v, :, pl.ds(c * LANES, LANES)] = value
    for copy, n in top_copies + slab_copies:
        copy.wait_send()
    for copy, sends, receives in edge_copies:
        pl.when(sends)(copy.wait_send)


def solution(mesh):
    ranges, slabs = mesh.shape["morton"], mesh.shape["group"]

    along_group = [(g, 0) for g in range(slabs - 1, 0, -1)]
    along_morton = [(0, r) for r in range(ranges - 1, 0, -1)]
    across = [(g, r) for g in range(slabs - 1, 0, -1) for r in range(ranges - 1, 0, -1)]
    phases = [across + along_group + along_morton] if ranges * slabs <= 64 else [along_morton, along_group]
    partners = sum(len(phase) for phase in phases)

    def per_device(state, patch_count, neighbour_table, send_table, ghost_table):
        _, slots, variables, count_cells = state.shape
        message = send_table.shape[2]
        tiles = count_cells // LANES
        f32 = jnp.float32
        vmem, smem, dma = pltpu.VMEM, pltpu.SMEM, pltpu.SemaphoreType.DMA
        state = jnp.transpose(state[0], (1, 0, 2))
        patch_count = patch_count.reshape(1, 1)
        neighbour_table = jnp.transpose(neighbour_table, (0, 2, 1))
        send_table = jnp.transpose(send_table, (2, 0, 1))
        ghost_table = jnp.transpose(ghost_table, (0, 2, 1))
        out = pl.pallas_call(
            functools.partial(kernel, ranges, slabs, phases, slots, message),
            out_shape=pltpu.VMEM(state.shape, f32),
            in_specs=[pl.BlockSpec(memory_space=pltpu.HBM)] * 5,
            out_specs=pl.BlockSpec(memory_space=pltpu.VMEM),
            scratch_shapes=[
                vmem(state.shape, f32),
                smem(patch_count.shape, jnp.int32),
                smem(neighbour_table.shape, jnp.int32),
                smem(send_table.shape, jnp.int32),
                smem(ghost_table.shape, jnp.int32),
                vmem((2 * slots, 8, LANES), f32),
                vmem((2 * slots, 8, LANES), f32),
                vmem((len(OFFSETS), message, 8, LANES), f32),
                vmem(((2 * REACH + 1) * message, 8, LANES), f32),
                vmem((2, (VARS + 1) // 2, slots, LANES), f32),
                vmem(((VARS + 1) // 2, slots, LANES), f32),
                vmem(((VARS + 1) // 2, slots, LANES), f32),
                vmem((2 * slots, 8, LANES), f32),
                vmem((2, 1, LANES), f32),
                vmem((partners, 1, LANES), f32),
                dma,
                dma((4,)),
                dma((len(OFFSETS),)),
                dma((len(OFFSETS),)),
                dma((2,)),
                dma((2,)),
                dma((partners,)),
                dma((partners,)),
            ],
            compiler_params=pltpu.CompilerParams(collective_id=0, has_side_effects=True),
        )(state, patch_count, neighbour_table, send_table, ghost_table)
        return jnp.transpose(out, (1, 0, 2))[None]

    placed = (
        P("group", "morton", None, None),
        P("morton"),
        P("morton", None, None),
        P("morton", None, None),
        P("morton", None, None),
    )
    return jax.shard_map(
        per_device,
        mesh=mesh,
        in_specs=placed,
        out_specs=P("group", "morton", None, None),
        check_vma=False,
    )
```
